32 devices in a mesh: eq: 2 (over x), row: 4 (over y, core), col: 4 (over z).
Axes of the slice: x: 2, y: 2, z: 4, core: 2. Of those that a mesh axis runs over, the one named last changes fastest.
Arguments:
- transition: float32 [6144, 3072], P(('eq', 'row'), 'col'), parts along dimension 0, may hold values from -0.05 to 0.9
- covariance: float32 [6144, 3072], P(('eq', 'row'), 'col'), parts along dimension 0, may hold values from -1 to 5, as said below
Outputs:
- covariance_out: float32 [6144, 3072], P(('eq', 'row'), 'col'), parts along dimension 0
- transition_out: float32 [6144, 3072], P(('eq', 'row'), 'col'), parts along dimension 0
The draws below stay inside these ranges and needn't reach their ends.
There are 2 independent parts, one for each index of `eq`. The reference program is written for one: setup_inputs(seed, part) draws one part's arguments, and reference() takes and returns one part's arrays. A program takes and returns all parts, laid end to end along the dimension named above; each array names one. Nothing has to cross between parts.
Inputs may be any that keep to these rules, and one draw needn't show every extreme that they name: covariance is exactly symmetric.
All inputs are finite; a program needn't handle non-finite values.
Results may differ from the reference program's by a relative error of at most 0.0001.
Values sent between devices are 32-bit elements; how exact they have to be, the bound alone decides.
No kernel may reach another device: no remote copies, remote signals or barrier semaphores. Data moves between devices by JAX's collectives and lax.ppermute only.
A program may use at most 128 MiB of HBM per device.

```python
import jax
import jax.numpy as jnp
from jax import lax

ORDER = 3072
STEPS = 1


def draw_transition(key, part):
    keys = jax.random.split(jax.random.fold_in(key, 11), 2)
    diagonal = jax.random.uniform(keys[0], (ORDER,), jnp.float32, 0.5, 0.85)
    noise = jnp.clip(jax.random.normal(keys[1], (ORDER, ORDER), jnp.float32), -6.0, 6.0) * (0.12 / ORDER ** 0.5)
    noise = jnp.clip(noise, -0.05, 0.05)
    return noise + jnp.diag(diagonal)


def draw_covariance(key, part):
    keys = jax.random.split(jax.random.fold_in(key, 23), 3)
    diagonal = jax.random.uniform(keys[0], (ORDER,), jnp.float32, 1.0, 3.0)
    normals = jnp.clip(jax.random.normal(keys[1], (ORDER, ORDER), jnp.float32), -6.0, 6.0)
    noise = jnp.clip(normals * (0.4 / (2.0 * ORDER) ** 0.5), -0.45, 0.45)
    result = noise + noise.T + jnp.diag(diagonal)
    return result


def setup_inputs(seed: int = 0, part: int = 0) -> dict:
    key_list = jax.random.split(jax.random.key(seed), 3)
    part_splits = jax.random.split(jax.random.fold_in(key_list[2], part), 3)
    transition = draw_transition(jax.random.fold_in(jax.random.fold_in(key_list[2], part), 71), part)
    covariance = draw_covariance(jax.random.fold_in(jax.random.fold_in(key_list[2], part), 71), part)
    return dict(transition=transition, covariance=covariance)


def reference(transition, covariance):
    highest = lax.Precision.HIGHEST
    matrix = transition
    current = covariance
    for repeat in range(STEPS):
        product = jnp.dot(matrix, current, precision=highest, preferred_element_type=jnp.float32)
        current = jnp.dot(product, matrix.T, precision=highest, preferred_element_type=jnp.float32) + current
        matrix = jnp.dot(matrix, matrix, precision=highest, preferred_element_type=jnp.float32)
    return current, matrix
```

```python
import jax
import jax.numpy as jnp
from jax import lax
from jax.sharding import PartitionSpec as P


CHUNKS = 2
PRECISION = lax.Precision.HIGH


def gather_rows(block, rows):
    if rows != 4:
        return lax.all_gather(block, "row", axis=0, tiled=True)
    far = lax.ppermute(block, "row", [(i, i ^ 2) for i in range(4)])
    near = lax.ppermute(block, "row", [(i, i ^ 1) for i in range(4)])
    both = lax.ppermute(far, "row", [(i, i ^ 1) for i in range(4)])
    return jnp.concatenate([block, near, far, both], axis=0)


def per_device(transition, covariance):
    cols = lax.axis_size("col")
    rows = lax.axis_size("row")
    k = lax.axis_index("col")
    place = lax.axis_index("row")
    height, width = transition.shape
    size = height // CHUNKS if height % (8 * CHUNKS) == 0 else height
    chunks = height // size

    def column(offset):
        return lax.rem(k + offset + cols, cols)

    def slot(index):
        if rows != 4:
            return index * width
        return lax.bitwise_xor(index, place) * width

    def dot(a, b, dim):
        return lax.dot_general(
            a, b, (((1,), (dim,)), ((), ())), precision=PRECISION, preferred_element_type=jnp.float32
        )

    x_column = gather_rows(covariance, rows)
    a_column = gather_rows(transition, rows)

    def gather_row(part):
        right = [part]
        left = [part]
        for s in range(1, cols):
            right.append(lax.ppermute(right[-1], "col", [(i, i + 1) for i in range(s - 1, cols - 1)]))
            left.append(lax.ppermute(left[-1], "col", [(i + 1, i) for i in range(cols - s)]))
        row = jnp.zeros((size, cols * width), part.dtype)
        row = lax.dynamic_update_slice_in_dim(row, part, slot(k), axis=1)
        for s in [2, 1, 3] if cols == 4 else range(1, cols):
            piece = jnp.where(k >= s, right[s], left[cols - s])
            row = lax.dynamic_update_slice_in_dim(row, piece, slot(column(-s)), axis=1)
        return row

    a_rows = [gather_row(transition[h * size : (h + 1) * size]) for h in range(chunks)]
    updated = []
    squared = []
    for h, a_row in enumerate(a_rows):
        product = dot(a_row, x_column, 0)
        partial = []
        for d in range(cols):
            block = lax.dynamic_slice_in_dim(a_column, slot(column(d)), width, axis=0)
            partial.append(dot(product, block, 1))
        total = covariance[h * size : (h + 1) * size] + partial[0]
        right = left = None
        for d in range(cols - 1, 0, -1):
            send = partial[d] if right is None else partial[d] + right
            right = lax.ppermute(send, "col", [(i, i + 1) for i in range(cols - d)])
            send = partial[cols - d] if left is None else partial[cols - d] + left
            left = lax.ppermute(send, "col", [(i, i - 1) for i in range(d, cols)])
        if right is not None:
            total = total + (right + left)
        updated.append(total)
        squared.append(dot(a_row, a_column, 0))
    return (jnp.concatenate(updated, axis=0), jnp.concatenate(squared, axis=0))


def solution(mesh):
    spec = P(("eq", "row"), "col")
    return jax.shard_map(per_device, mesh=mesh, in_specs=(spec, spec), out_specs=(spec, spec), check_vma=False)
```
